128 devices in a mesh: ao: 16 (over x, y), aux: 8 (over z, core).
Axes of the slice: x: 4, y: 4, z: 4, core: 2. Of those that a mesh axis runs over, the one named last changes fastest.
Arguments:
- blocks: bfloat16 [96, 512, 128, 128], P('ao', 'aux'), may hold values from -6 to 6
- pairs: int32 [96, 2], P('ao'), may hold values from 0 to 159, as said below
- counts: int32 [16], P('ao'), may hold values from 1 to 6, as said below
- owned_blocks: int32 [160], P('ao'), may hold values from 0 to 159, as said below
- occ_coef: bfloat16 [160, 8, 128], P('ao'), may hold values from -0.5 to 0.5
- vir_coef: bfloat16 [20480, 18432], P('ao', 'aux'), may hold values from -0.078125 to 0.078125
Outputs:
- b_tensor: bfloat16 [512, 8, 18432], P('ao', None, 'aux')
The draws below stay inside these ranges and needn't reach their ends.
Inputs may be any that keep to these rules, and one draw needn't show every extreme that they name: `pairs`: among the used slots of one ao index, at most 3 have nu blocks whose rows one owner holds; in every draw some index reaches 3. `counts`: some ao index uses all 6 slots in every draw. `owned_blocks`: every atom block appears exactly once.
All inputs are finite; a program needn't handle non-finite values.
Results may differ from the reference program's by a relative error of at most 0.014.
Values may be sent and summed in bfloat16 or wider, within the bound.
A program may use at most 128 MiB of HBM per device.

```python
import jax
import jax.numpy as jnp
from jax import lax

BLK = 128
BLK_DEV = 10
OCC = 8
SLOTS = 6
NBLK = 160
NAO = 20480
PS = 512
V = 18432
CAP = 3
ALL_SLOTS = 96
N_AO = 16


def slot_layout(key):
    perm_blocks = jax.random.permutation(jax.random.fold_in(key, 11), NBLK).astype(jnp.int32)
    used_counts = jax.random.randint(jax.random.fold_in(key, 12), (N_AO,), 1, SLOTS + 1).astype(jnp.int32)
    full_index = jax.random.randint(jax.random.fold_in(key, 13), (), 0, N_AO)
    used_counts = jnp.where(jnp.arange(N_AO) == full_index, SLOTS, used_counts).astype(jnp.int32)
    first_owner = jax.random.randint(jax.random.fold_in(key, 14), (N_AO,), 0, N_AO)
    second_owner = (first_owner + 1 + jax.random.randint(jax.random.fold_in(key, 15), (N_AO,), 0, N_AO - 1)) % N_AO
    slot_half = jnp.arange(SLOTS) // CAP
    owner_pick = jnp.where(slot_half[None, :] == 0, first_owner[:, None], second_owner[:, None])
    local_pick = jax.random.randint(jax.random.fold_in(key, 16), (N_AO, SLOTS), 0, BLK_DEV)
    second_block = perm_blocks[owner_pick * BLK_DEV + local_pick]
    first_block = jax.random.randint(jax.random.fold_in(key, 17), (N_AO, SLOTS), 0, NBLK)
    pair_list = jnp.stack([first_block, second_block], axis=-1).reshape(N_AO * SLOTS, 2).astype(jnp.int32)
    return (pair_list, used_counts, perm_blocks)


def draw_pairs(key, part):
    return slot_layout(key)[0]


def draw_counts(key, part):
    return slot_layout(key)[1]


def draw_owned_blocks(key, part):
    return slot_layout(key)[2]


def steps_of(stream_key, extent, shards, low, top_value):
    factor_of, own = 1.0, jax.random.fold_in(stream_key, 6)
    for axis_at, shards_of in shards:
        draws = jnp.exp(jax.random.uniform(jax.random.fold_in(own, axis_at), (shards_of,), jnp.float32, low / len(shards), top_value / len(shards)))
        factor_of = factor_of * jnp.repeat(draws, extent[axis_at] // shards_of).reshape([-1 if axis == axis_at else 1 for axis in range(len(extent))])
    return factor_of


def scatter_about(rng, shape, width, bound, pieces=(), kind=jnp.bfloat16):
    array = jax.random.normal(rng, shape, jnp.float32) * width
    if len(pieces) > 0:
        array = steps_of(rng, shape, pieces, -0.22, 0.18) * array
    return jnp.clip(array, min=-bound, max=bound).astype(kind)


def setup_inputs(seed: int = 0) -> dict:
    streams_of = jax.random.split(jax.random.key(seed), 7)
    blocks = scatter_about(streams_of[0], (ALL_SLOTS, PS, BLK, BLK), 1.0, 6.0, ((0, 16), (1, 8)))
    pairs = draw_pairs(jax.random.fold_in(streams_of[6], 71), 0)
    counts = draw_counts(jax.random.fold_in(streams_of[6], 71), 0)
    owned_blocks = draw_owned_blocks(jax.random.fold_in(streams_of[6], 71), 0)
    occ_coef = scatter_about(streams_of[4], (NBLK, OCC, BLK), BLK ** -0.5, 0.5, ((0, 16),))
    vir_coef = scatter_about(streams_of[5], (NAO, V), (BLK * ALL_SLOTS // 2) ** -0.5, 0.078125, ((0, 16), (1, 8)))
    return {"blocks": blocks, "pairs": pairs, "counts": counts, "owned_blocks": owned_blocks, "occ_coef": occ_coef, "vir_coef": vir_coef}


def half_slab(args):
    block, coef, in_use = args
    value = jnp.einsum("im,pmn->pin", coef.astype(jnp.float32), block.astype(jnp.float32))
    return jnp.where(in_use, value, jnp.zeros_like(value)).astype(jnp.bfloat16)


def reference(blocks, pairs, counts, owned_blocks, occ_coef, vir_coef):
    total_blocks = owned_blocks.shape[0]
    slot_total = pairs.shape[0]
    slot_count = slot_total // N_AO
    block_width = blocks.shape[2]
    positions = jnp.arange(total_blocks, dtype=jnp.int32)
    place = jnp.zeros((total_blocks,), jnp.int32).at[owned_blocks].set(positions)
    in_use = (jnp.arange(slot_count, dtype=jnp.int32)[None, :] < counts[:, None]).reshape(-1)
    row_first = place[pairs[:, 0]]
    row_second = place[pairs[:, 1]]
    slabs = lax.map(half_slab, (blocks, occ_coef[row_first], in_use))
    gathered = jax.ops.segment_sum(slabs.astype(jnp.float32), row_second, num_segments=total_blocks)
    gathered = gathered.astype(jnp.bfloat16)
    per_owner = total_blocks // N_AO
    occupied = occ_coef.shape[1]
    total = jnp.zeros((PS * occupied, vir_coef.shape[1]), jnp.float32)
    for owner_idx in range(N_AO):
        part = gathered[owner_idx * per_owner:(owner_idx + 1) * per_owner]
        left = jnp.transpose(part, (1, 2, 0, 3)).reshape(PS * occupied, per_owner * block_width)
        right = vir_coef[owner_idx * per_owner * block_width:(owner_idx + 1) * per_owner * block_width]
        term = jnp.dot(left, right, preferred_element_type=jnp.float32).astype(jnp.bfloat16)
        total = total + term.astype(jnp.float32)
    return total.reshape(PS, occupied, vir_coef.shape[1]).astype(jnp.bfloat16)
```

```python
import functools

import jax
import jax.numpy as jnp
from jax import lax
from jax.experimental import pallas as pl
from jax.experimental.pallas import tpu as pltpu
from jax.sharding import PartitionSpec as P

MESH = pl.DeviceIdType.MESH
VMEM = pltpu.VMEM
DMA = pltpu.SemaphoreType.DMA


def greet(peers):
    barrier = pltpu.get_barrier_semaphore()
    for peer in peers:
        pl.semaphore_signal(barrier, inc=1, device_id=peer, device_id_type=MESH)
    pl.semaphore_wait(barrier, len(peers))


def remote(src, dst, send_sem, recv_sem, peer):
    return pltpu.make_async_remote_copy(
        src_ref=src, dst_ref=dst, send_sem=send_sem, recv_sem=recv_sem,
        device_id=peer, device_id_type=MESH,
    )


def tables_kernel(groups, ints_ref, occ_ref, ints_all, occ_all, send, recv):
    me = lax.axis_index("ao")
    peers = [{"ao": lax.rem(me + k, groups)} for k in range(1, groups)]
    greet(peers)
    copies = []
    for k, peer in enumerate(peers):
        copies.append(remote(ints_ref, ints_all.at[me], send.at[0, k], recv.at[0, k], peer))
        copies.append(remote(occ_ref, occ_all.at[me], send.at[1, k], recv.at[1, k], peer))
    for copy in copies:
        copy.start()
    ints_all[me] = ints_ref[...]
    occ_all[me] = occ_ref[...]
    for copy in copies:
        copy.wait()


def regroup_kernel(groups, per_owner, half_ref, pick_ref, out_ref, got, parts, send, recv):
    me = lax.axis_index("ao")
    peers = [{"ao": lax.rem(me + k, groups)} for k in range(1, groups)]
    rows = half_ref.shape[2]
    mine = pl.ds(pl.multiple_of(me * rows, 16), rows)
    greet(peers)
    copies = []
    for k, peer in enumerate(peers):
        copies.append(
            remote(half_ref.at[peer["ao"]], got.at[:, mine, :], send.at[0, k], recv.at[0, k], peer)
        )
    for copy in copies:
        copy.start()
    got[:, mine, :] = half_ref[me]
    for copy in copies:
        copy.wait_recv()
    owner_rows = per_owner * 8
    slot = lax.rem(me, 8) * 2 + me // 8

    def summed(owner, dst):
        pick = pick_ref[pl.ds(pl.multiple_of(owner * owner_rows, 16), owner_rows), :]
        for u in range(2):
            both = jnp.concatenate([got[2 * u], got[2 * u + 1]], axis=1)
            total = jnp.dot(pick, both, preferred_element_type=jnp.float32)
            for l in range(per_owner):
                tile = jnp.concatenate(
                    [total[8 * l:8 * l + 8, :128], total[8 * l:8 * l + 8, 128:]], axis=0
                )
                dst[16 * u:16 * u + 16, 128 * l:128 * l + 128] = tile.astype(jnp.bfloat16)

    def handed(k):
        owner = lax.rem(me + k, groups)
        return remote(parts.at[owner], out_ref.at[slot], send.at[1, k - 1], recv.at[1, k - 1], {"ao": owner})

    def step(k, carry):
        owner = lax.rem(me + k, groups)
        summed(owner, parts.at[owner])

        @pl.when(k > 1)
        def _():
            handed(k - 1).start()

        return carry

    lax.fori_loop(1, groups, step, 0)
    summed(me, out_ref.at[slot])
    handed(groups - 1).start()
    for copy in copies:
        copy.wait_send()

    def finish(k, carry):
        handed(k).wait()
        return carry

    lax.fori_loop(1, groups, finish, 0)


def product_kernel(
    chunks, left_ref, vir_hbm, out_ref, vir, left, part,
    got1, got2, got3, got4, vir_sem,
    c_send, c_recv, s1_send, s1_recv, s2_send, s2_recv, s3_send, s3_recv, s4_send, s4_recv,
):
    ao, aux = lax.axis_index("ao"), lax.axis_index("aux")
    x, y = ao // 4, lax.rem(ao, 4)
    z, core = aux // 2, lax.rem(aux, 2)

    def turn(v, by):
        return lax.rem(v + by + 4, 4)

    def at_xy(xx, yy):
        return {"ao": xx * 4 + yy}

    def at_z(zz, cc):
        return {"aux": zz * 2 + cc}

    up, down, other = at_z(turn(z, 1), core), at_z(turn(z, -1), core), at_z(z, 1 - core)
    near = [
        [[at_xy(turn(x, 1), y), at_xy(turn(x, -1), y)], [at_xy(x, turn(y, 1)), at_xy(x, turn(y, -1))]],
        [[at_xy(x, turn(y, 1)), at_xy(x, turn(y, -1))], [at_xy(turn(x, 1), y), at_xy(turn(x, -1), y)]],
    ]
    major, minor = [x, y], [y, x]
    sides = (1, -1)
    load = pltpu.make_async_copy(vir_hbm, vir, vir_sem)
    load.start()
    greet([up, down, other] + near[0][0] + near[0][1])

    unit = left_ref.shape[1]
    mid = unit // 2

    def rows_of(index, start=0, size=unit):
        return pl.ds(pl.multiple_of(index * unit + start, 16), size)

    def left_copy(q, k, src, rows, peer):
        return remote(src, left.at[q, rows], c_send.at[k, q], c_recv.at[k, q], peer)

    def index_of(zz, cc):
        return zz * 2 + cc

    def own_copy(q, k):
        peer = (up, down, other)[k]
        return left_copy(q, k, left_ref.at[q], rows_of(aux), peer)

    def half_copy(q, k):
        zz = turn(z, -1) if k == 0 else turn(z, 1)
        rows = rows_of(index_of(zz, core), mid * k, mid)
        return left_copy(q, 3 + k, left.at[q, rows], rows, (up, down)[k])

    def side_copy(q, k):
        zz = turn(z, (-1, 1, 2)[k])
        rows = rows_of(index_of(zz, core))
        return left_copy(q, 5 + k, left.at[q, rows], rows, other)

    def gather_start(q):
        for k in range(3):
            own_copy(q, k).start()
        left[q, rows_of(aux)] = left_ref[q]

    def gather_near(q):
        for k in range(2):
            own_copy(q, k).wait_recv()
            half_copy(q, k).start()
            side_copy(q, k).start()

    def gather_far(q):
        for k in range(2):
            half_copy(q, k).wait_recv()
        side_copy(q, 2).start()

    def gather_wait(q):
        own_copy(q, 2).wait_recv()
        for k in range(3):
            side_copy(q, k).wait_recv()

    def multiply(q):
        def tile(n, carry):
            cols = pl.ds(pl.multiple_of(n * 256, 256), 256)
            term = jnp.dot(left[q], vir[:, cols], preferred_element_type=jnp.float32)
            part[q, :, :, :, :, cols] = term.astype(jnp.bfloat16).reshape(4, 4, 2, 16, 256)
            return carry

        lax.fori_loop(0, vir.shape[1] // 256, tile, 0)

    def slab(q, f, a, b):
        return part.at[q, a, b, 0] if f == 0 else part.at[q, b, a, 1]

    half_cols = vir.shape[1] // 2

    def copy1(q, f, d):
        return remote(
            slab(q, f, turn(major[f], 2), pl.ds(2 * d, 2)), got1.at[f, d, q],
            s1_send.at[f, d, q], s1_recv.at[f, d, q], near[f][0][d],
        )

    def copy2(q, f, d):
        return remote(
            slab(q, f, turn(major[f], sides[d]), pl.ds(0, 4)), got2.at[f, d, q],
            s2_send.at[f, d, q], s2_recv.at[f, d, q], near[f][0][d],
        )

    def copy3(q, f, d):
        return remote(
            slab(q, f, major[f], turn(minor[f], 2)).at[:, pl.ds(d * half_cols, half_cols)], got3.at[f, d, q],
            s3_send.at[f, d, q], s3_recv.at[f, d, q], near[f][1][d],
        )

    def copy4(q, f, d):
        return remote(
            slab(q, f, major[f], turn(minor[f], sides[d])), got4.at[f, d, q],
            s4_send.at[f, d, q], s4_recv.at[f, d, q], near[f][1][d],
        )

    pairs = [(f, d) for f in range(2) for d in range(2)]

    def wide(v):
        return v.astype(jnp.float32)

    def stage1(q):
        for f, d in pairs:
            copy1(q, f, d).start()

    def stage2(q):
        for f, d in pairs:
            copy1(q, f, d).wait_recv()
            mine = slab(q, f, turn(major[f], sides[d]), pl.ds(2 * d, 2))
            mine[...] = (wide(mine[...]) + wide(got1[f, d, q])).astype(jnp.bfloat16)
            copy2(q, f, d).start()

    def stage3(q):
        for f in range(2):
            for d in range(2):
                copy2(q, f, d).wait_recv()
            for j in (2, 1, 3, 0):
                b = turn(minor[f], j)
                mine = slab(q, f, major[f], b)
                mine[...] = (
                    wide(mine[...]) + wide(got2[f, 0, q, b]) + wide(got2[f, 1, q, b])
                ).astype(jnp.bfloat16)
            for d in range(2):
                copy3(q, f, d).start()

    def stage4(q):
        for f, d in pairs:
            copy3(q, f, d).wait_recv()
            mine = slab(q, f, major[f], turn(minor[f], sides[d])).at[:, pl.ds(d * half_cols, half_cols)]
            mine[...] = (wide(mine[...]) + wide(got3[f, d, q])).astype(jnp.bfloat16)
            copy4(q, f, d).start()

    def stage5(q):
        for f in range(2):
            for d in range(2):
                copy4(q, f, d).wait_recv()
            mine = slab(q, f, major[f], minor[f])
            out_ref[pl.ds(pl.multiple_of(q * 32 + f * 16, 16), 16), :] = (
                wide(mine[...]) + wide(got4[f, 0, q]) + wide(got4[f, 1, q])
            ).astype(jnp.bfloat16)

    gather_start(0)
    gather_start(1)
    gather_near(0)
    gather_start(2)
    gather_near(1)
    gather_far(0)
    load.wait()

    def step(it, carry):
        def on(q, work):
            @pl.when(jnp.logical_and(q >= 0, q < chunks))
            def _():
                work(q)

        on(it, gather_wait)
        on(it, multiply)
        on(it, stage1)
        on(it + 3, gather_start)
        on(it + 2, gather_near)
        on(it - 1, stage2)
        on(it + 1, gather_far)
        on(it - 2, stage3)
        on(it - 3, stage4)
        on(it - 4, stage5)
        return carry

    lax.fori_loop(0, chunks + 4, step, 0)

    def finish(q, carry):
        for k in range(3):
            own_copy(q, k).wait_send()
            side_copy(q, k).wait_send()
        for k in range(2):
            half_copy(q, k).wait_send()
        for f, d in pairs:
            copy1(q, f, d).wait_send()
            copy2(q, f, d).wait_send()
            copy3(q, f, d).wait_send()
            copy4(q, f, d).wait_send()
        return carry

    lax.fori_loop(0, chunks, finish, 0)


def params(collective_id, vmem=None):
    return pltpu.CompilerParams(
        collective_id=collective_id, has_side_effects=True, vmem_limit_bytes=vmem
    )


def block_place(block_ids, owned_all):
    hits = block_ids[..., None] == owned_all
    positions = jnp.arange(owned_all.shape[0], dtype=jnp.int32)
    return jnp.sum(jnp.where(hits, positions, 0), axis=-1)


def per_device(blocks, pairs, counts, owned_blocks, occ_coef, vir_coef):
    groups = lax.axis_size("ao")
    slots, depth, _, width = blocks.shape
    occupied = occ_coef.shape[1]
    per_owner = owned_blocks.shape[0]
    cols = vir_coef.shape[1]
    bf16, i32 = jnp.bfloat16, jnp.int32
    spec = pl.BlockSpec(memory_space=VMEM)

    n_ints = per_owner + 2 * slots + 1
    ints = jnp.concatenate([owned_blocks, pairs[:, 0], pairs[:, 1], counts])
    ints = jnp.pad(ints[None, :], ((0, 7), (0, 128 - n_ints)))
    ints_all, occ_all = pl.pallas_call(
        functools.partial(tables_kernel, groups),
        out_shape=(
            jax.ShapeDtypeStruct((groups, 8, 128), i32),
            jax.ShapeDtypeStruct((groups, per_owner * occupied, width), bf16),
        ),
        in_specs=[spec] * 2,
        out_specs=(spec, spec),
        scratch_shapes=[DMA((2, groups - 1)), DMA((2, groups - 1))],
        compiler_params=params(0),
    )(ints, occ_coef.reshape(per_owner * occupied, width))

    ints_all = ints_all[:, 0, :n_ints]
    owned_all = ints_all[:, :per_owner].reshape(-1)
    second_all = ints_all[:, per_owner + slots:per_owner + 2 * slots]
    live = jnp.arange(slots, dtype=i32)[None, :] < ints_all[:, n_ints - 1:]
    second_all = jnp.where(live, second_all, -1).reshape(-1)
    orbital = jnp.arange(occupied, dtype=i32)
    rows = (owned_all[:, None] * occupied + orbital).reshape(-1)
    hits = (jnp.where(second_all < 0, -occupied, second_all * occupied)[:, None] + orbital).reshape(-1)
    pick = (rows[:, None] == hits[None, :]).astype(bf16)

    occ_all = occ_all.reshape(groups * per_owner, occupied, width)
    occ_pick = occ_all[block_place(pairs[:, 0], owned_all)]
    half = jnp.einsum("sim,spmn->psin", occ_pick, blocks, preferred_element_type=jnp.float32)
    in_use = jnp.arange(slots, dtype=i32) < counts[0]
    half = jnp.where(in_use[None, :, None, None], half, 0.0).astype(bf16)
    half = half.reshape(groups, depth // groups, slots * occupied, width)

    piece = depth // groups * occupied
    left = pl.pallas_call(
        functools.partial(regroup_kernel, groups, per_owner),
        out_shape=jax.ShapeDtypeStruct((groups, piece, per_owner * width), bf16),
        in_specs=[spec] * 2,
        out_specs=spec,
        scratch_shapes=[
            VMEM((depth // groups, groups * slots * occupied, width), bf16),
            VMEM((groups, piece, per_owner * width), bf16),
            DMA((2, groups - 1)),
            DMA((2, groups - 1)),
        ],
        compiler_params=params(1),
    )(half, pick)

    chunks = 8
    left = left.reshape(chunks, 2 * piece, per_owner * width)
    sems = [DMA((8, chunks)), DMA((8, chunks))] + [DMA((2, 2, chunks))] * 8
    out = pl.pallas_call(
        functools.partial(product_kernel, chunks),
        out_shape=jax.ShapeDtypeStruct((groups * 16, cols), bf16),
        in_specs=[spec, pl.BlockSpec(memory_space=pl.ANY)],
        out_specs=spec,
        scratch_shapes=[
            VMEM(vir_coef.shape, bf16),
            VMEM((chunks, 8 * 2 * piece, per_owner * width), bf16),
            VMEM((chunks, 4, 4, 2, 16, cols), bf16),
            VMEM((2, 2, chunks, 2, 16, cols), bf16),
            VMEM((2, 2, chunks, 4, 16, cols), bf16),
            VMEM((2, 2, chunks, 16, cols // 2), bf16),
            VMEM((2, 2, chunks, 16, cols), bf16),
            DMA,
        ] + sems,
        compiler_params=params(2, 66 * 1024 * 1024 - 3 * 1024 * 1024),
    )(left, vir_coef)
    return out.reshape(-1, occupied, cols)


def solution(mesh):
    in_specs = (
        P("ao", "aux", None, None),
        P("ao", None),
        P("ao"),
        P("ao"),
        P("ao", None, None),
        P("ao", "aux"),
    )
    out_specs = P("ao", None, "aux")
    return jax.shard_map(
        per_device, mesh=mesh, in_specs=in_specs, out_specs=out_specs, check_vma=False
    )
```

```python
import functools

import jax
import jax.numpy as jnp
from jax import lax
from jax.experimental import pallas as pl
from jax.experimental.pallas import tpu as pltpu
from jax.sharding import PartitionSpec as P

MESH = pl.DeviceIdType.MESH
VMEM = pltpu.VMEM
DMA = pltpu.SemaphoreType.DMA


def greet(peers):
    barrier = pltpu.get_barrier_semaphore()
    for peer in peers:
        pl.semaphore_signal(barrier, inc=1, device_id=peer, device_id_type=MESH)
    pl.semaphore_wait(barrier, len(peers))


def remote(src, dst, send_sem, recv_sem, peer):
    return pltpu.make_async_remote_copy(
        src_ref=src, dst_ref=dst, send_sem=send_sem, recv_sem=recv_sem,
        device_id=peer, device_id_type=MESH,
    )


def tables_kernel(groups, ints_ref, occ_ref, ints_all, occ_all, send, recv):
    me = lax.axis_index("ao")
    peers = [{"ao": lax.rem(me + k, groups)} for k in range(1, groups)]
    greet(peers)
    copies = []
    for k, peer in enumerate(peers):
        copies.append(remote(ints_ref, ints_all.at[me], send.at[0, k], recv.at[0, k], peer))
        copies.append(remote(occ_ref, occ_all.at[me], send.at[1, k], recv.at[1, k], peer))
    for copy in copies:
        copy.start()
    ints_all[me] = ints_ref[...]
    occ_all[me] = occ_ref[...]
    for copy in copies:
        copy.wait()


def product_kernel(
    groups, chunks, depth, half_ref, pick_ref, vir_hbm, out_ref, got, parts, owned, vir, left, part,
    got1, got2, got3, got4, vir_sem, p1_send, p1_recv, p2_send, p2_recv,
    c_send, c_recv, s1_send, s1_recv, s2_send, s2_recv, s3_send, s3_recv, s4_send, s4_recv,
):
    ao, aux = lax.axis_index("ao"), lax.axis_index("aux")
    x, y = ao // 4, lax.rem(ao, 4)
    z, core = aux // 2, lax.rem(aux, 2)

    def turn(v, by):
        return lax.rem(v + by + 4, 4)

    def at_xy(xx, yy):
        return {"ao": xx * 4 + yy}

    def at_z(zz, cc):
        return {"aux": zz * 2 + cc}

    up, down, other = at_z(turn(z, 1), core), at_z(turn(z, -1), core), at_z(z, 1 - core)
    near = [
        [[at_xy(turn(x, 1), y), at_xy(turn(x, -1), y)], [at_xy(x, turn(y, 1)), at_xy(x, turn(y, -1))]],
        [[at_xy(x, turn(y, 1)), at_xy(x, turn(y, -1))], [at_xy(turn(x, 1), y), at_xy(turn(x, -1), y)]],
    ]
    major, minor = [x, y], [y, x]
    sides = (1, -1)
    load = pltpu.make_async_copy(vir_hbm, vir, vir_sem)
    load.start()
    greet([up, down, other] + [{"ao": lax.rem(ao + k, groups)} for k in range(1, groups)])

    rows = half_ref.shape[2]
    mine = pl.ds(pl.multiple_of(ao * rows, 16), rows)

    def piece_copy(s, k):
        peer = lax.rem(ao + k, groups)
        return remote(
            half_ref.at[peer, pl.ds(2 * s, 2)], got.at[pl.ds(2 * s, 2), mine, :],
            p1_send.at[s, k - 1], p1_recv.at[s, k - 1], {"ao": peer},
        )

    def slot_of(s):
        start = pl.multiple_of(ao // 8 * 32 + lax.rem(ao, 2) * 16, 16)
        return owned.at[s * 4 + lax.rem(ao, 8) // 2, pl.ds(start, 16), :]

    def block_copy(s, k):
        peer = lax.rem(ao + k, groups)
        return remote(
            parts.at[s, peer], slot_of(s), p2_send.at[s, k - 1], p2_recv.at[s, k - 1], {"ao": peer}
        )

    per_owner = left.shape[2] // 128
    group_rows = 4 * per_owner * 8

    def sum_blocks(s):
        both = jnp.concatenate([got[2 * s], got[2 * s + 1]], axis=1)

        def hand(xx):
            for j in range(4):
                k = lax.rem(xx * 4 + j - ao + groups, groups)

                @pl.when(k > 0)
                def _():
                    block_copy(s, k).start()

        for g in range(4):
            xx = turn(x, g + 1)
            pick = pick_ref[pl.ds(pl.multiple_of(xx * group_rows, 16), group_rows), :]
            total = jnp.dot(pick, both, preferred_element_type=jnp.float32)
            for j in range(4):
                for l in range(per_owner):
                    at = (j * per_owner + l) * 8
                    tile = jnp.concatenate([total[at:at + 8, :128], total[at:at + 8, 128:]], axis=0)
                    parts[s, xx * 4 + j, :, 128 * l:128 * l + 128] = tile.astype(jnp.bfloat16)
            if g > 0:
                hand(turn(x, g))
        slot_of(s)[...] = parts[s, ao]
        hand(x)

    def each_peer(work):
        def step(k, carry):
            work(k)
            return carry

        lax.fori_loop(1, groups, step, 0)

    for s in range(2):
        each_peer(lambda k: piece_copy(s, k).start())
    got[:, mine, :] = half_ref[ao]
    for s in range(2):
        each_peer(lambda k: piece_copy(s, k).wait_recv())
        sum_blocks(s)

    unit = owned.shape[1]
    mid = unit // 2

    def rows_of(index, start=0, size=unit):
        return pl.ds(pl.multiple_of(index * unit + start, 16), size)

    def left_copy(q, k, src, rows, peer):
        return remote(src, left.at[q, rows], c_send.at[k, q], c_recv.at[k, q], peer)

    def index_of(zz, cc):
        return zz * 2 + cc

    def own_copy(q, k):
        peer = (up, down, other)[k]
        return left_copy(q, k, owned.at[q], rows_of(aux), peer)

    def half_copy(q, k):
        zz = turn(z, -1) if k == 0 else turn(z, 1)
        rows = rows_of(index_of(zz, core), mid * k, mid)
        return left_copy(q, 3 + k, left.at[q, rows], rows, (up, down)[k])

    def side_copy(q, k):
        zz = turn(z, (-1, 1, 2)[k])
        rows = rows_of(index_of(zz, core))
        return left_copy(q, 5 + k, left.at[q, rows], rows, other)

    def gather_start(q):
        for k in range(3):
            own_copy(q, k).start()
        left[q, rows_of(aux)] = owned[q]

    def gather_near(q):
        for k in range(2):
            own_copy(q, k).wait_recv()
            half_copy(q, k).start()
            side_copy(q, k).start()

    def gather_far(q):
        for k in range(2):
            half_copy(q, k).wait_recv()
        side_copy(q, 2).start()

    def gather_wait(q):
        own_copy(q, 2).wait_recv()
        for k in range(3):
            side_copy(q, k).wait_recv()

    def multiply(q):
        def tile(n, carry):
            cols = pl.ds(pl.multiple_of(n * 256, 256), 256)
            term = jnp.dot(left[q], vir[:, cols], preferred_element_type=jnp.float32)
            part[lax.rem(q, depth), :, :, :, :, cols] = term.astype(jnp.bfloat16).reshape(4, 4, 2, 16, 256)
            return carry

        lax.fori_loop(0, vir.shape[1] // 256, tile, 0)

    def slab(q, f, a, b):
        q = lax.rem(q, depth)
        return part.at[q, a, b, 0] if f == 0 else part.at[q, b, a, 1]

    half_cols = vir.shape[1] // 2

    def copy1(q, f, d):
        return remote(
            slab(q, f, turn(major[f], 2), pl.ds(2 * d, 2)), got1.at[f, d, q],
            s1_send.at[f, d, q], s1_recv.at[f, d, q], near[f][0][d],
        )

    def copy2(q, f, d):
        return remote(
            slab(q, f, turn(major[f], sides[d]), pl.ds(0, 4)), got2.at[f, d, q],
            s2_send.at[f, d, q], s2_recv.at[f, d, q], near[f][0][d],
        )

    def copy3(q, f, d):
        return remote(
            slab(q, f, major[f], turn(minor[f], 2)).at[:, pl.ds(d * half_cols, half_cols)], got3.at[f, d, q],
            s3_send.at[f, d, q], s3_recv.at[f, d, q], near[f][1][d],
        )

    def copy4(q, f, d):
        return remote(
            slab(q, f, major[f], turn(minor[f], sides[d])), got4.at[f, d, q],
            s4_send.at[f, d, q], s4_recv.at[f, d, q], near[f][1][d],
        )

    pairs = [(f, d) for f in range(2) for d in range(2)]

    def wide(v):
        return v.astype(jnp.float32)

    def stage1(q):
        for f, d in pairs:
            copy1(q, f, d).start()

    def stage2(q):
        for f, d in pairs:
            copy1(q, f, d).wait_recv()
            mine = slab(q, f, turn(major[f], sides[d]), pl.ds(2 * d, 2))
            mine[...] = (wide(mine[...]) + wide(got1[f, d, q])).astype(jnp.bfloat16)
            copy2(q, f, d).start()

    def stage3(q):
        for f in range(2):
            for d in range(2):
                copy2(q, f, d).wait_recv()
            for j in (2, 1, 3, 0):
                b = turn(minor[f], j)
                mine = slab(q, f, major[f], b)
                mine[...] = (
                    wide(mine[...]) + wide(got2[f, 0, q, b]) + wide(got2[f, 1, q, b])
                ).astype(jnp.bfloat16)
            for d in range(2):
                copy3(q, f, d).start()

    def stage4(q):
        for f, d in pairs:
            copy3(q, f, d).wait_recv()
            mine = slab(q, f, major[f], turn(minor[f], sides[d])).at[:, pl.ds(d * half_cols, half_cols)]
            mine[...] = (wide(mine[...]) + wide(got3[f, d, q])).astype(jnp.bfloat16)
            copy4(q, f, d).start()

    def stage5(q):
        for f in range(2):
            for d in range(2):
                copy4(q, f, d).wait_recv()
            mine = slab(q, f, major[f], minor[f])
            row = lax.rem(q, 4) * 64 + f * 32 + q // 4 * 16
            out_ref[pl.ds(pl.multiple_of(row, 16), 16), :] = (
                wide(mine[...]) + wide(got4[f, 0, q]) + wide(got4[f, 1, q])
            ).astype(jnp.bfloat16)

    def release(q):
        for f, d in pairs:
            copy1(q, f, d).wait_send()
            copy2(q, f, d).wait_send()
            copy3(q, f, d).wait_send()
            copy4(q, f, d).wait_send()

    each_peer(lambda k: block_copy(0, k).wait_recv())
    gather_start(0)
    gather_start(1)
    gather_near(0)
    gather_start(2)
    gather_near(1)
    gather_far(0)
    load.wait()

    def step(it, carry):
        def on(q, work):
            @pl.when(jnp.logical_and(q >= 0, q < chunks))
            def _():
                work(q)

        on(it, gather_wait)
        on(it, multiply)
        on(it, stage1)

        @pl.when(it == 1)
        def _():
            each_peer(lambda k: block_copy(1, k).wait_recv())

        on(it + 3, gather_start)
        on(it + 2, gather_near)
        on(it - 1, stage2)
        on(it + 1, gather_far)
        on(it - 2, stage3)
        on(it - 3, stage4)
        on(it - 4, stage5)
        on(it - 5, release)
        return carry

    lax.fori_loop(0, chunks + 5, step, 0)

    def finish(q, carry):
        for k in range(3):
            own_copy(q, k).wait_send()
            side_copy(q, k).wait_send()
        for k in range(2):
            half_copy(q, k).wait_send()
        return carry

    lax.fori_loop(0, chunks, finish, 0)
    for s in range(2):
        each_peer(lambda k: piece_copy(s, k).wait_send())
        each_peer(lambda k: block_copy(s, k).wait_send())


def params(collective_id, vmem=None):
    return pltpu.CompilerParams(
        collective_id=collective_id, has_side_effects=True, vmem_limit_bytes=vmem
    )


def block_place(block_ids, owned_all):
    hits = block_ids[..., None] == owned_all
    positions = jnp.arange(owned_all.shape[0], dtype=jnp.int32)
    return jnp.sum(jnp.where(hits, positions, 0), axis=-1)


def per_device(blocks, pairs, counts, owned_blocks, occ_coef, vir_coef):
    groups = lax.axis_size("ao")
    slots, depth, _, width = blocks.shape
    occupied = occ_coef.shape[1]
    per_owner = owned_blocks.shape[0]
    cols = vir_coef.shape[1]
    bf16, i32 = jnp.bfloat16, jnp.int32
    spec = pl.BlockSpec(memory_space=VMEM)

    n_ints = per_owner + 2 * slots + 1
    ints = jnp.concatenate([owned_blocks, pairs[:, 0], pairs[:, 1], counts])
    ints = jnp.pad(ints[None, :], ((0, 7), (0, 128 - n_ints)))
    ints_all, occ_all = pl.pallas_call(
        functools.partial(tables_kernel, groups),
        out_shape=(
            jax.ShapeDtypeStruct((groups, 8, 128), i32),
            jax.ShapeDtypeStruct((groups, per_owner * occupied, width), bf16),
        ),
        in_specs=[spec] * 2,
        out_specs=(spec, spec),
        scratch_shapes=[DMA((2, groups - 1)), DMA((2, groups - 1))],
        compiler_params=params(0),
    )(ints, occ_coef.reshape(per_owner * occupied, width))

    ints_all = ints_all[:, 0, :n_ints]
    owned_all = ints_all[:, :per_owner].reshape(-1)
    second_all = ints_all[:, per_owner + slots:per_owner + 2 * slots]
    live = jnp.arange(slots, dtype=i32)[None, :] < ints_all[:, n_ints - 1:]
    second_all = jnp.where(live, second_all, -1).reshape(-1)
    orbital = jnp.arange(occupied, dtype=i32)
    rows = (owned_all[:, None] * occupied + orbital).reshape(-1)
    hits = (jnp.where(second_all < 0, -occupied, second_all * occupied)[:, None] + orbital).reshape(-1)
    pick = (rows[:, None] == hits[None, :]).astype(bf16)

    occ_all = occ_all.reshape(groups * per_owner, occupied, width)
    occ_pick = occ_all[block_place(pairs[:, 0], owned_all)]
    half = jnp.einsum("sim,spmn->psin", occ_pick, blocks, preferred_element_type=jnp.float32)
    in_use = jnp.arange(slots, dtype=i32) < counts[0]
    half = jnp.where(in_use[None, :, None, None], half, 0.0).astype(bf16)
    half = half.reshape(groups, depth // groups, slots * occupied, width)

    chunks, slots_deep = 8, 6
    wide = per_owner * width
    half_sems = [DMA((2, groups - 1))] * 4
    sems = [DMA((8, chunks)), DMA((8, chunks))] + [DMA((2, 2, chunks))] * 8
    out = pl.pallas_call(
        functools.partial(product_kernel, groups, chunks, slots_deep),
        out_shape=jax.ShapeDtypeStruct((groups * 16, cols), bf16),
        in_specs=[spec, spec, pl.BlockSpec(memory_space=pl.ANY)],
        out_specs=spec,
        scratch_shapes=[
            VMEM((depth // groups, groups * slots * occupied, width), bf16),
            VMEM((2, groups, 16, wide), bf16),
            VMEM((chunks, 64, wide), bf16),
            VMEM(vir_coef.shape, bf16),
            VMEM((chunks, 8 * 64, wide), bf16),
            VMEM((slots_deep, 4, 4, 2, 16, cols), bf16),
            VMEM((2, 2, chunks, 2, 16, cols), bf16),
            VMEM((2, 2, chunks, 4, 16, cols), bf16),
            VMEM((2, 2, chunks, 16, cols // 2), bf16),
            VMEM((2, 2, chunks, 16, cols), bf16),
            DMA,
        ] + half_sems + sems,
        compiler_params=params(1, 63 * 1024 * 1024),
    )(half, pick, vir_coef)
    return out.reshape(-1, occupied, cols)


def solution(mesh):
    in_specs = (
        P("ao", "aux", None, None),
        P("ao", None),
        P("ao"),
        P("ao"),
        P("ao", None, None),
        P("ao", "aux"),
    )
    out_specs = P("ao", None, "aux")
    return jax.shard_map(
        per_device, mesh=mesh, in_specs=in_specs, out_specs=out_specs, check_vma=False
    )
```
